32 devices in a mesh: grp: 2 (over x), rep: 8 (over z, y), blk: 2 (over core).
Axes of the slice: x: 2, y: 2, z: 4, core: 2. Of those that a mesh axis runs over, the one named last changes fastest.
Arguments:
- factors: float32 [16, 1280, 1280], P('grp', ('blk', 'rep')), as said below
- damping: float32 [16], P('grp'), may hold values from 0.1 to 1
Outputs:
- root: float32 [16, 1280, 1280], P('grp', ('blk', 'rep'))
- inv_root: float32 [16, 1280, 1280], P('grp', ('blk', 'rep'))
The draws below stay inside these ranges and needn't reach their ends.
Inputs may be any that keep to these rules, and one draw needn't show every extreme that they name: `factors`: every factor is symmetric positive semidefinite.
All inputs are finite; a program needn't handle non-finite values.
Results may differ from the reference program's by a relative error of at most 0.0035.
The reference program's roundings to bfloat16 on the way (of `step_mat`) count: a program that leaves them out, or rounds other values in their place, can miss the bound.
Values may be sent and summed in bfloat16 or wider, within the bound.
No kernel may reach another device: no remote copies, remote signals or barrier semaphores. Data moves between devices by JAX's collectives and lax.ppermute only.
A program may use at most 128 MiB of HBM per device.

```python
import math
import jax
import jax.numpy as jnp
from jax import lax

N = 1280
ITERS = 4
FACTORS = 16


def draw_factors(key, part):
    mix_key, scale_key = jax.random.split(jax.random.fold_in(key, 11))
    mixing = jax.random.normal(mix_key, (FACTORS, N, N), jnp.float32)
    spectrum = jnp.exp(jax.random.uniform(scale_key, (FACTORS, N), jnp.float32, jnp.log(0.001), jnp.log(10.0)))
    weighted = mixing * spectrum[:, None, :]
    product = jnp.einsum('fik,fjk->fij', weighted, mixing, precision=lax.Precision.HIGHEST) / N
    return 0.5 * (product + jnp.swapaxes(product, 1, 2))


def levels(rng, dims, pieces, least, top_value):
    def one(position, blocks):
        steps = jax.random.uniform(jax.random.fold_in(jax.random.fold_in(rng, 6), position), (blocks,), jnp.float32, least / len(pieces), top_value / len(pieces))
        return jnp.repeat(jnp.exp(steps), dims[position] // blocks).reshape((-1,) + (1,) * (len(dims) - position - 1))

    loudness = one(*pieces[0])
    for cut in pieces[1:]:
        loudness = loudness * one(*cut)
    return loudness


def setup_inputs(seed: int = 0) -> dict:
    key_of = jax.random.split(jax.random.key(seed), 3)
    factors = draw_factors(jax.random.fold_in(key_of[2], 71), 0)
    damping = jnp.clip(jnp.exp(math.log(1.0) - 2.3025851 * jax.random.uniform(key_of[1], (FACTORS,), jnp.float32) ** levels(key_of[1], (FACTORS,), ((0, 2),), -0.2, 0.2)), 0.1, 1.0)
    return dict(factors=factors, damping=damping)


def one_factor(factor_pair):
    factor, damp_value = factor_pair
    identity = jnp.eye(N, dtype=jnp.float32)
    damped = factor + damp_value * identity
    frob_norm = jnp.sqrt(jnp.sum(damped * damped))
    iterate = (damped / frob_norm).astype(jnp.bfloat16)
    inverse = identity.astype(jnp.bfloat16)
    for sweep_idx in range(ITERS):
        moment = jnp.dot(inverse, iterate, preferred_element_type=jnp.float32)
        step_mat = ((3.0 * identity - moment) * 0.5).astype(jnp.bfloat16)
        new_iterate = jnp.dot(iterate, step_mat, preferred_element_type=jnp.float32).astype(jnp.bfloat16)
        inverse = jnp.dot(step_mat, inverse, preferred_element_type=jnp.float32).astype(jnp.bfloat16)
        iterate = new_iterate
    root_scale = jnp.sqrt(frob_norm)
    return (iterate.astype(jnp.float32) * root_scale, inverse.astype(jnp.float32) / root_scale)

def reference(factors, damping):
    root, inv_root = lax.map(one_factor, (factors, damping))
    return (root, inv_root)
```

```python
import jax
import jax.numpy as jnp
from jax import lax
from jax.sharding import PartitionSpec as P

ITERS = 4


def per_device(factors, damping):
    fac_grp, row_count, order_full = factors.shape
    rep_count = lax.axis_size("rep")
    fac_rep = fac_grp // rep_count
    blk_rows = row_count * rep_count
    blk_idx = lax.axis_index("blk")
    rep_idx = lax.axis_index("rep")
    col_ids = lax.iota(jnp.int32, order_full)
    row_ids = blk_idx * blk_rows + rep_idx * row_count + lax.iota(jnp.int32, row_count)
    eye_block = (row_ids[:, None] == col_ids[None, :]).astype(jnp.float32)
    damped = factors + damping[:, None, None] * eye_block[None, :, :]
    factor_norms = jnp.sqrt(lax.psum(jnp.sum(damped * damped, axis=(1, 2)), ("rep", "blk")))
    scaled = (damped / factor_norms[:, None, None]).astype(jnp.bfloat16)
    scaled = scaled.reshape(rep_count, fac_rep, row_count, order_full)
    own = lax.all_to_all(scaled, "rep", split_axis=0, concat_axis=0, tiled=True)
    iterate = jnp.swapaxes(own, 0, 1).reshape(fac_rep, blk_rows, order_full)

    iter_rows = blk_idx * blk_rows + lax.iota(jnp.int32, blk_rows)
    eye_rows = (iter_rows[:, None] == col_ids[None, :]).astype(jnp.float32)[None]
    swap = ((0, 1), (1, 0))

    def own_cols(mat):
        return lax.dynamic_slice_in_dim(mat, blk_idx * blk_rows, blk_rows, 2)

    def peer_cols(mat):
        return lax.dynamic_slice_in_dim(mat, (1 - blk_idx) * blk_rows, blk_rows, 2)

    def rows_times(left, right_rows):
        peer_rows = lax.ppermute(right_rows, "blk", swap)
        first = jnp.einsum(
            "fik,fkj->fij", own_cols(left), right_rows, preferred_element_type=jnp.float32
        )
        second = jnp.einsum(
            "fik,fkj->fij", peer_cols(left), peer_rows, preferred_element_type=jnp.float32
        )
        return first + second

    step_rows = ((3.0 * eye_rows - iterate.astype(jnp.float32)) * 0.5).astype(jnp.bfloat16)
    iterate = rows_times(iterate, step_rows).astype(jnp.bfloat16)
    inverse = step_rows
    for sweep_idx in range(1, ITERS):
        moment = rows_times(inverse, iterate)
        step_rows = ((3.0 * eye_rows - moment) * 0.5).astype(jnp.bfloat16)
        both = jnp.concatenate([iterate, inverse], axis=1)
        both = rows_times(both, step_rows).astype(jnp.bfloat16)
        iterate, inverse = both[:, :blk_rows], both[:, blk_rows:]

    def send_back(mat):
        blocks = mat.reshape(fac_rep, rep_count, row_count, order_full)
        blocks = jnp.swapaxes(blocks, 0, 1)
        back = lax.all_to_all(blocks, "rep", split_axis=0, concat_axis=0, tiled=True)
        return back.reshape(fac_grp, row_count, order_full).astype(jnp.float32)

    root_scale = jnp.sqrt(factor_norms)[:, None, None]
    return (send_back(iterate) * root_scale, send_back(inverse) / root_scale)


def solution(mesh):
    return jax.shard_map(
        per_device,
        mesh=mesh,
        in_specs=(P("grp", ("blk", "rep"), None), P("grp")),
        out_specs=(P("grp", ("blk", "rep"), None), P("grp", ("blk", "rep"), None)),
        check_vma=False,
    )
```

```python
import jax
import jax.numpy as jnp
from jax import lax
from jax.sharding import PartitionSpec as P

ITERS = 4


def per_device(factors, damping):
    fac_grp, row_count, order_full = factors.shape
    rep_count = lax.axis_size("rep")
    fac_rep = fac_grp // rep_count
    blk_rows = row_count * rep_count
    blk_idx = lax.axis_index("blk")
    rep_idx = lax.axis_index("rep")
    col_ids = lax.iota(jnp.int32, order_full)
    row_ids = blk_idx * blk_rows + rep_idx * row_count + lax.iota(jnp.int32, row_count)
    eye_block = (row_ids[:, None] == col_ids[None, :]).astype(jnp.float32)
    damped = factors + damping[:, None, None] * eye_block[None, :, :]
    swap = ((0, 1), (1, 0))

    def across(mat, mask):
        return lax.ppermute(mat, "rep", [(dev, dev ^ mask) for dev in range(rep_count)])

    squares = jnp.sum(damped * damped, axis=(1, 2))
    squares = squares + lax.ppermute(squares, "blk", swap)
    mask = 1
    while mask < rep_count:
        squares = squares + across(squares, mask)
        mask *= 2
    factor_norms = jnp.sqrt(squares)
    scaled = (damped / factor_norms[:, None, None]).astype(jnp.bfloat16)
    scaled = scaled.reshape(rep_count, fac_rep, row_count, order_full)
    own = lax.all_to_all(scaled, "rep", split_axis=0, concat_axis=0, tiled=True)
    iterate = jnp.swapaxes(own, 0, 1).reshape(fac_rep, blk_rows, order_full)

    iter_rows = blk_idx * blk_rows + lax.iota(jnp.int32, blk_rows)
    eye_rows = (iter_rows[:, None] == col_ids[None, :]).astype(jnp.float32)[None]

    def own_cols(mat):
        return lax.dynamic_slice_in_dim(mat, blk_idx * blk_rows, blk_rows, 2)

    def peer_cols(mat):
        return lax.dynamic_slice_in_dim(mat, (1 - blk_idx) * blk_rows, blk_rows, 2)

    def peer_of(rows):
        return lax.ppermute(rows, "blk", swap)

    def rows_times(left, right_rows, peer_rows):
        first = jnp.einsum(
            "fik,fkj->fij", own_cols(left), right_rows, preferred_element_type=jnp.float32
        )
        second = jnp.einsum(
            "fik,fkj->fij", peer_cols(left), peer_rows, preferred_element_type=jnp.float32
        )
        return first + second

    step_rows = ((3.0 * eye_rows - iterate.astype(jnp.float32)) * 0.5).astype(jnp.bfloat16)
    iterate = rows_times(iterate, step_rows, peer_of(step_rows)).astype(jnp.bfloat16)
    inverse = step_rows
    for sweep_idx in range(1, ITERS):
        moment = rows_times(inverse, iterate, peer_of(iterate))
        step_rows = ((3.0 * eye_rows - moment) * 0.5).astype(jnp.bfloat16)
        peer_step = peer_of(step_rows)
        if sweep_idx < ITERS - 1:
            both = jnp.concatenate([iterate, inverse], axis=1)
            both = rows_times(both, step_rows, peer_step).astype(jnp.bfloat16)
            iterate, inverse = both[:, :blk_rows], both[:, blk_rows:]
        else:
            iterate = rows_times(iterate, step_rows, peer_step).astype(jnp.bfloat16)
            inverse = rows_times(inverse, step_rows, peer_step).astype(jnp.bfloat16)

    root_scale = jnp.sqrt(factor_norms).reshape(rep_count, fac_rep, 1, 1)

    def send_back(mat, rescale):
        blocks = mat.reshape(fac_rep, rep_count, row_count, order_full)
        whole = jnp.zeros((rep_count, fac_rep, row_count, order_full), jnp.float32)
        for mask in reversed(range(rep_count)):
            mate = rep_idx ^ mask
            block = lax.dynamic_index_in_dim(blocks, mate, 1, keepdims=False)
            if mask:
                block = across(block, mask)
            scale = lax.dynamic_index_in_dim(root_scale, mate, 0, keepdims=False)
            block = rescale(block.astype(jnp.float32), scale)
            whole = lax.dynamic_update_index_in_dim(whole, block, mate, 0)
        return whole.reshape(fac_grp, row_count, order_full)

    return (
        send_back(iterate, lambda block, scale: block * scale),
        send_back(inverse, lambda block, scale: block / scale),
    )


def solution(mesh):
    return jax.shard_map(
        per_device,
        mesh=mesh,
        in_specs=(P("grp", ("blk", "rep"), None), P("grp")),
        out_specs=(P("grp", ("blk", "rep"), None), P("grp", ("blk", "rep"), None)),
        check_vma=False,
    )
```

```python
import jax
import jax.numpy as jnp
from jax import lax
from jax.sharding import PartitionSpec as P

ITERS = 4


def per_device(factors, damping):
    fac_grp, row_count, order_full = factors.shape
    rep_count = lax.axis_size("rep")
    fac_rep = fac_grp // rep_count
    blk_rows = row_count * rep_count
    blk_idx = lax.axis_index("blk")
    rep_idx = lax.axis_index("rep")
    col_ids = lax.iota(jnp.int32, order_full)
    row_ids = blk_idx * blk_rows + rep_idx * row_count + lax.iota(jnp.int32, row_count)
    eye_block = (row_ids[:, None] == col_ids[None, :]).astype(jnp.float32)
    damped = factors + damping[:, None, None] * eye_block[None, :, :]
    swap = ((0, 1), (1, 0))

    def across(mat, mask):
        return lax.ppermute(mat, "rep", [(dev, dev ^ mask) for dev in range(rep_count)])

    squares = jnp.sum(damped * damped, axis=(1, 2))
    squares = squares + lax.ppermute(squares, "blk", swap)
    mask = 1
    while mask < rep_count:
        squares = squares + across(squares, mask)
        mask *= 2
    factor_norms = jnp.sqrt(squares)
    scaled = (damped / factor_norms[:, None, None]).astype(jnp.bfloat16)
    scaled = scaled.reshape(rep_count, fac_rep, row_count, order_full)
    own = jnp.zeros_like(scaled)
    for mask in reversed(range(rep_count)):
        block = lax.dynamic_index_in_dim(scaled, rep_idx ^ mask, 0, keepdims=False)
        if mask:
            block = across(block, mask)
        own = lax.dynamic_update_index_in_dim(own, block, rep_idx ^ mask, 0)
    iterate = jnp.swapaxes(own, 0, 1).reshape(fac_rep, blk_rows, order_full)

    iter_rows = blk_idx * blk_rows + lax.iota(jnp.int32, blk_rows)
    eye_rows = (iter_rows[:, None] == col_ids[None, :]).astype(jnp.float32)[None]

    def own_cols(mat):
        return lax.dynamic_slice_in_dim(mat, blk_idx * blk_rows, blk_rows, 2)

    def peer_cols(mat):
        return lax.dynamic_slice_in_dim(mat, (1 - blk_idx) * blk_rows, blk_rows, 2)

    def peer_of(rows):
        return lax.ppermute(rows, "blk", swap)

    def rows_times(left, right_rows, peer_rows):
        first = jnp.einsum(
            "fik,fkj->fij", own_cols(left), right_rows, preferred_element_type=jnp.float32
        )
        second = jnp.einsum(
            "fik,fkj->fij", peer_cols(left), peer_rows, preferred_element_type=jnp.float32
        )
        return first + second

    step_rows = ((3.0 * eye_rows - iterate.astype(jnp.float32)) * 0.5).astype(jnp.bfloat16)
    iterate = rows_times(iterate, step_rows, peer_of(step_rows)).astype(jnp.bfloat16)
    inverse = step_rows
    for sweep_idx in range(1, ITERS):
        moment = rows_times(inverse, iterate, peer_of(iterate))
        step_rows = ((3.0 * eye_rows - moment) * 0.5).astype(jnp.bfloat16)
        peer_step = peer_of(step_rows)
        if sweep_idx < ITERS - 1:
            both = jnp.concatenate([iterate, inverse], axis=1)
            both = rows_times(both, step_rows, peer_step).astype(jnp.bfloat16)
            iterate, inverse = both[:, :blk_rows], both[:, blk_rows:]
        else:
            iterate = rows_times(iterate, step_rows, peer_step).astype(jnp.bfloat16)
            inverse = rows_times(inverse, step_rows, peer_step).astype(jnp.bfloat16)

    root_scale = jnp.sqrt(factor_norms).reshape(rep_count, fac_rep, 1, 1)

    def send_back(mat, rescale):
        blocks = mat.reshape(fac_rep, rep_count, row_count, order_full)
        whole = jnp.zeros((rep_count, fac_rep, row_count, order_full), jnp.float32)
        for mask in reversed(range(rep_count)):
            mate = rep_idx ^ mask
            block = lax.dynamic_index_in_dim(blocks, mate, 1, keepdims=False)
            if mask:
                block = across(block, mask)
            scale = lax.dynamic_index_in_dim(root_scale, mate, 0, keepdims=False)
            block = rescale(block.astype(jnp.float32), scale)
            whole = lax.dynamic_update_index_in_dim(whole, block, mate, 0)
        return whole.reshape(fac_grp, row_count, order_full)

    return (
        send_back(iterate, lambda block, scale: block * scale),
        send_back(inverse, lambda block, scale: block / scale),
    )


def solution(mesh):
    return jax.shard_map(
        per_device,
        mesh=mesh,
        in_specs=(P("grp", ("blk", "rep"), None), P("grp")),
        out_specs=(P("grp", ("blk", "rep"), None), P("grp", ("blk", "rep"), None)),
        check_vma=False,
    )
```
